256 devices in a mesh: gz: 64 (over z, x, core), col: 4 (over y).
Axes of the slice: x: 4, y: 4, z: 8, core: 2. Of those that a mesh axis runs over, the one named last changes fastest.
Arguments:
- source: float32 [4096, 2048], P('gz', 'col'), may hold values from -6 to 6
- z_vectors: float32 [4096, 4096], P('gz', 'col'), may hold values from -0.25 to 0.25
- x_vectors: float32 [4, 4], replicated, may hold values from -3 to 3
- y_vectors: float32 [512, 512], replicated, may hold values from -0.25 to 0.25
- z_values: float32 [4096], replicated, may hold values from 0.1 to 3
- x_values: float32 [4], replicated, may hold values from 0.1 to 3
- y_values: float32 [512], replicated, may hold values from 0.1 to 3
Outputs:
- solution: float32 [4096, 2048], P('gz', 'col')
The draws below stay inside these ranges and needn't reach their ends.
All inputs are finite; a program needn't handle non-finite values.
Results may differ from the reference program's by a relative error of at most 0.000092.
Values sent between devices are 32-bit elements; how exact they have to be, the bound alone decides.
No kernel may reach another device: no remote copies, remote signals or barrier semaphores. Data moves between devices by JAX's collectives and lax.ppermute only.
A program may use at most 64 MiB of HBM per device.

```python
import math
import jax
import jax.numpy as jnp
from jax import lax

NY = 512
NZ = 4096
NX = 4


def strengthened(drawn, own_key, source, target, blocks, factor):
    owner, partner = [(jnp.arange(drawn.shape[dim]) // (drawn.shape[dim] // blocks)).reshape([-1 if axis == dim else 1 for axis in range(drawn.ndim)]) for dim in (source, target)]
    chosen = jax.random.permutation(own_key, blocks)[partner]
    strong = (owner == chosen) | (owner == (partner + blocks // 2) % blocks)
    return jnp.where(strong, factor * drawn, drawn)


def level_of(stream_key, extent, split, low, top_value):
    def one(dim, blocks):
        draws = jax.random.uniform(jax.random.fold_in(jax.random.fold_in(stream_key, 6), dim), (blocks,), jnp.float32, low / len(split), top_value / len(split))
        return jnp.repeat(jnp.exp(draws), extent[dim] // blocks).reshape((-1,) + (1,) * (len(extent) - dim - 1))

    level = one(*split[0])
    for cut in split[1:]:
        level = level * one(*cut)
    return level


def gaussian(rng, extent, width, reach, split=(), held_as=jnp.bfloat16):
    factor_of = level_of(rng, extent, split, -0.22, 0.18) if split else 1.0
    entries = jax.random.normal(rng, extent, jnp.float32) * width * factor_of
    return jnp.minimum(jnp.maximum(entries, -reach), reach).astype(held_as)


def noise_with(own_key, dims, spread, most, cuts, heavy, held_as=jnp.bfloat16):
    values = spread * jax.random.normal(own_key, dims, jnp.float32)
    if cuts:
        values = values * level_of(own_key, dims, cuts, -0.22, 0.18)
    return jnp.clip(strengthened(values, jax.random.fold_in(own_key, 3), *heavy), -most, most).astype(held_as)


def setup_inputs(seed: int = 0) -> dict:
    splits = jax.random.split(jax.random.key(seed), 8)
    source = gaussian(splits[0], (NZ, NX * NY), 1.0, 6.0, ((0, 64), (1, 4)), jnp.float32)
    z_vectors = noise_with(splits[1], (NZ, NZ), NZ ** -0.5, 0.25, ((0, 64), (1, 4)), (0, 1, 64, 4.0), jnp.float32)
    x_vectors = gaussian(splits[2], (NX, NX), NX ** -0.5, 3.0, (), jnp.float32)
    y_vectors = gaussian(splits[3], (NY, NY), NY ** -0.5, 0.25, (), jnp.float32)
    z_values = jnp.clip(jnp.exp(jax.random.uniform(splits[4], (NZ,), jnp.float32, math.log(0.1), math.log(3.0))), 0.1, 3.0)
    x_values = jnp.clip(jnp.exp(jax.random.uniform(splits[5], (NX,), jnp.float32, math.log(0.1), math.log(3.0))), 0.1, 3.0)
    y_values = jnp.clip(jnp.exp(jax.random.uniform(splits[6], (NY,), jnp.float32, math.log(0.1), math.log(3.0))), 0.1, 3.0)
    return dict(source=source, z_vectors=z_vectors, x_vectors=x_vectors, y_vectors=y_vectors, z_values=z_values, x_values=x_values, y_values=y_values)


def reference(source, z_vectors, x_vectors, y_vectors, z_values, x_values, y_values):
    exact_mode = lax.Precision.HIGHEST
    field = source.reshape(NZ, NX, NY)
    along_y = jnp.einsum("zxy,yj->zxj", field, y_vectors, precision=exact_mode)
    along_x = jnp.einsum("zxj,xi->zij", along_y, x_vectors, precision=exact_mode)
    flat_modes = along_x.reshape(NZ, NX * NY)
    coefficients = lax.dot_general(z_vectors, flat_modes, (((0,), (0,)), ((), ())), precision=exact_mode, preferred_element_type=jnp.float32)
    divisor = z_values[:, None, None] + x_values[None, :, None] + y_values[None, None, :]
    scaled = coefficients.reshape(NZ, NX, NY) / divisor
    back_z = jnp.dot(z_vectors, scaled.reshape(NZ, NX * NY), precision=exact_mode, preferred_element_type=jnp.float32)
    back_x = jnp.einsum("zij,xi->zxj", back_z.reshape(NZ, NX, NY), x_vectors, precision=exact_mode)
    solution = jnp.einsum("zxj,yj->zxy", back_x, y_vectors, precision=exact_mode)
    return solution.reshape(NZ, NX * NY)
```

```python
import functools
import jax
import jax.numpy as jnp
from jax import lax
from jax.experimental import pallas as pl
from jax.experimental.pallas import tpu as pltpu
from jax.sharding import Mesh
from jax.sharding import PartitionSpec as P

NZ_CHIPS, NX_CHIPS, CORES, NY_CHIPS = 8, 4, 2, 4
GZ = ("z", "x", "core")
SIZE = {"z": NZ_CHIPS, "x": NX_CHIPS, "core": CORES, "y": NY_CHIPS}
OFFSETS = (0, -1, -2, -3, 4, 1, 2, 3)


VMEM = pl.BlockSpec(memory_space=pltpu.VMEM)
SMEM = pl.BlockSpec(memory_space=pltpu.SMEM)


def f32(*shape):
    return jax.ShapeDtypeStruct(shape, jnp.float32)


def bf16(*shape):
    return jax.ShapeDtypeStruct(shape, jnp.bfloat16)


def shifted(value, axis, step):
    n = SIZE[axis]
    return lax.ppermute(value, axis, [(i, (i + step) % n) for i in range(n)])


def two_parts(value):
    high = value.astype(jnp.bfloat16)
    return high, (value - high.astype(jnp.float32)).astype(jnp.bfloat16)


def product(left, right, dims):
    one = functools.partial(
        lax.dot_general, dimension_numbers=(dims, ((), ())), preferred_element_type=jnp.float32
    )
    (lh, ll), (rh, rl) = left, right
    return one(lh, rh) + (one(ll, rh) + one(lh, rl))


NN = ((1,), (0,))
NT = ((1,), (1,))


def left_lanes(like):
    return lax.broadcasted_iota(jnp.int32, like.shape, 1) < 64


def swapped_in(a, b):
    left = left_lanes(a)
    return jnp.where(left, a, pltpu.roll(b, 64, 1)), jnp.where(left, pltpu.roll(a, 64, 1), b)


def along_y_kernel(source, y_vectors, packed):
    along_y = product(two_parts(source[...]), two_parts(y_vectors[...]), NN)
    for g in range(NZ_CHIPS // 2):
        lanes = slice(128 * g, 128 * g + 128)
        even, odd = swapped_in(along_y[:32, lanes], along_y[32:, lanes])
        packed[2 * g] = even
        packed[2 * g + 1] = odd


def forward_kernel(where, x_vectors, *refs):
    zs, (p0, p1, p2, p3), (to_partner, kept, z_high, z_low), (field,) = (
        refs[:9], refs[9:13], refs[13:17], refs[17:]
    )
    z, core, y = where[0], where[2], where[3]
    planes = (p0, p1, p2, p3)
    for p, offset in enumerate(OFFSETS):
        rows = slice(64 * p, 64 * p + 64)
        if offset == 4:
            for half, ref in ((0, zs[p]), (32, zs[8])):
                part = slice(64 * p + half, 64 * p + half + 32)
                z_high[part], z_low[part] = two_parts(ref[...])
        else:
            z_high[rows], z_low[rows] = two_parts(zs[p][...])
        block = lax.rem(z + NZ_CHIPS + offset, NZ_CHIPS)
        mine = [plane[block] for plane in planes]
        mixed = []
        for i in range(4):
            total = None
            for s in range(4):
                x = lax.rem(y + NY_CHIPS - s, NY_CHIPS)
                term = x_vectors[x, i] * mine[s]
                total = term if total is None else total + term
            mixed.append(total)
        for pair in range(2):
            top, bottom = swapped_in(mixed[2 * pair], mixed[2 * pair + 1])
            lanes = slice(128 * pair, 128 * pair + 128)
            field[64 * p : 64 * p + 32, lanes] = top
            field[64 * p + 32 : 64 * p + 64, lanes] = bottom
    turned = two_parts(field[...].T)
    for out, half in ((to_partner, 1 - core), (kept, core)):
        for tile in range(2):
            lanes = pl.ds(pl.multiple_of(half * 512 + tile * 256, 256), 256)
            out[:, 256 * tile : 256 * tile + 256] = product(
                turned, (z_high[:, lanes], z_low[:, lanes]), NN
            )


def by_owner_kernel(where, kept, received, *outs):
    for s, out in enumerate(outs):
        owner = lax.rem(where[1] + s, NX_CHIPS)
        lanes = pl.ds(pl.multiple_of(owner * 128, 128), 128)
        out[...] = kept[:, lanes] + received[:, lanes]


def scaled_kernel(a, b, c, d, divisor, out):
    out[...] = ((a[...] + b[...]) + (c[...] + d[...])) / divisor[...]


def backward_kernel(where, x_vectors, z_high, z_low, *refs):
    blocks, outs, (s_high, s_low) = refs[:8], refs[8:12], refs[12:]
    z, x, core, y = where[0], where[1], where[2], where[3]
    for partner in range(2):
        for s in range(NX_CHIPS):
            owner = lax.rem(x + NX_CHIPS - s, NX_CHIPS)
            half = core if partner == 0 else 1 - core
            lanes = pl.ds(pl.multiple_of(half * 512 + owner * 128, 128), 128)
            s_high[:, lanes], s_low[:, lanes] = two_parts(blocks[4 * partner + s][...])
    modes = (s_high[...], s_low[...])
    for p, offset in enumerate(OFFSETS):
        rows = slice(64 * p, 64 * p + 64)
        part = product((z_high[rows], z_low[rows]), modes, NT)
        block = lax.rem(z + NZ_CHIPS + offset, NZ_CHIPS)
        packed = []
        for pair in range(2):
            lanes = slice(128 * pair, 128 * pair + 128)
            packed += swapped_in(part[:32, lanes], part[32:, lanes])
        for s, out in enumerate(outs):
            x_out = lax.rem(y + s, NY_CHIPS)
            total = None
            for i in range(4):
                term = x_vectors[x_out, i] * packed[i]
                total = term if total is None else total + term
            out[block] = total


def along_y_back_kernel(packed, y_vectors, out, field):
    for g in range(NZ_CHIPS // 2):
        lanes = slice(128 * g, 128 * g + 128)
        field[:32, lanes], field[32:, lanes] = swapped_in(packed[2 * g], packed[2 * g + 1])
    out[...] = product(two_parts(field[...]), two_parts(y_vectors[...]), NT)


def call(kernel, out_shape, operands, smem=0, scratch=(), flops=0, name=None):
    outs = out_shape if isinstance(out_shape, (tuple, list)) else (out_shape,)
    moved = sum(a.size * a.dtype.itemsize for a in (*operands, *outs))
    return pl.pallas_call(
        kernel,
        out_shape=out_shape,
        in_specs=[SMEM] * smem + [VMEM] * (len(operands) - smem),
        out_specs=VMEM if outs is not out_shape else [VMEM] * len(outs),
        scratch_shapes=list(scratch),
        cost_estimate=pl.CostEstimate(flops=flops, bytes_accessed=moved, transcendentals=0),
        name=name,
    )(*operands)


def shards(source, z_vectors, x_vectors, y_vectors, z_values, x_values, y_values):
    z, x, core, y = (lax.axis_index(a) for a in ("z", "x", "core", "y"))
    where = jnp.stack([z, x, core, y]).astype(jnp.int32)

    z_part = lax.dynamic_slice_in_dim(z_values, y * 1024 + core * 512 + x * 128, 128)
    y_part = lax.dynamic_slice_in_dim(y_values, z * 64, 64)
    divisor = (z_part[None, None, :] + x_values[:, None, None]) + y_part[None, :, None]
    divisor = divisor.reshape(256, 128)

    right, left = [z_vectors], [z_vectors]
    for _ in range(3):
        right.append(shifted(right[-1], "z", 1))
        left.append(shifted(left[-1], "z", -1))
    far_top = shifted(right[3][:32], "z", 1)
    far_bottom = shifted(left[3][32:], "z", -1)
    z_blocks = (*right, far_top, *left[1:], far_bottom)

    packed = call(along_y_kernel, f32(8, 32, 128), (source, y_vectors), flops=2 * 64 * 512 * 512 * 3)
    plane = lax.all_to_all(packed, "z", 0, 0, tiled=True)
    planes = [plane] + [shifted(plane, "y", s) for s in (1, 2, 3)]

    to_partner, kept, z_high, z_low = call(
        forward_kernel,
        (f32(256, 512), f32(256, 512), bf16(512, 1024), bf16(512, 1024)),
        (where, x_vectors, *z_blocks, *planes),
        smem=2,
        scratch=[pltpu.VMEM((512, 256), jnp.float32)],
        flops=2 * 512 * 256 * 1024 * 3,
    )
    received = shifted(to_partner, "core", 1)
    mine, *others = call(by_owner_kernel, (f32(256, 128),) * 4, (where, kept, received), smem=1)
    sums = [shifted(part, "x", s) for s, part in enumerate(others, 1)]
    scaled = call(scaled_kernel, f32(256, 128), (mine, *sums, divisor))

    modes = [scaled] + [shifted(scaled, "x", s) for s in (1, 2, 3)]
    modes += [shifted(block, "core", 1) for block in modes]
    mine, *others = call(
        backward_kernel,
        (f32(8, 32, 128),) * 4,
        (where, x_vectors, z_high, z_low, *modes),
        smem=2,
        scratch=[pltpu.VMEM((256, 1024), jnp.bfloat16)] * 2,
        flops=2 * 512 * 256 * 1024 * 3,
    )
    for s, part in enumerate(others, 1):
        mine = mine + shifted(part, "y", s)
    back = lax.all_to_all(mine, "z", 0, 0, tiled=True)
    return call(
        along_y_back_kernel,
        f32(64, 512),
        (back, y_vectors),
        scratch=[pltpu.VMEM((64, 512), jnp.float32)],
        flops=2 * 64 * 512 * 512 * 3,
    )


def solution(mesh):
    devices = mesh.devices.reshape(NZ_CHIPS, NX_CHIPS, CORES, NY_CHIPS)
    torus = Mesh(devices, ("z", "x", "core", "y"))
    return jax.shard_map(
        shards,
        mesh=torus,
        in_specs=(P(GZ, "y"), P(GZ, "y"), P(), P(), P(), P(), P()),
        out_specs=P(GZ, "y"),
        check_vma=False,
    )
```

```python
import functools
import jax
import jax.numpy as jnp
from jax import lax
from jax.experimental import pallas as pl
from jax.experimental.pallas import tpu as pltpu
from jax.sharding import Mesh
from jax.sharding import PartitionSpec as P

NZ_CHIPS, NX_CHIPS, CORES, NY_CHIPS = 8, 4, 2, 4
GZ = ("z", "x", "core")
SIZE = {"z": NZ_CHIPS, "x": NX_CHIPS, "core": CORES, "y": NY_CHIPS}
OFFSETS = (4, 0, -1, -2, -3, 1, 2, 3)


VMEM = pl.BlockSpec(memory_space=pltpu.VMEM)
SMEM = pl.BlockSpec(memory_space=pltpu.SMEM)


def f32(*shape):
    return jax.ShapeDtypeStruct(shape, jnp.float32)


def bf16(*shape):
    return jax.ShapeDtypeStruct(shape, jnp.bfloat16)


def shifted(value, axis, step):
    n = SIZE[axis]
    return lax.ppermute(value, axis, [(i, (i + step) % n) for i in range(n)])


def two_parts(value):
    high = value.astype(jnp.bfloat16)
    return high, (value - high.astype(jnp.float32)).astype(jnp.bfloat16)


def product(left, right, dims):
    one = functools.partial(
        lax.dot_general, dimension_numbers=(dims, ((), ())), preferred_element_type=jnp.float32
    )
    (lh, ll), (rh, rl) = left, right
    return one(lh, rh) + (one(ll, rh) + one(lh, rl))


NN = ((1,), (0,))
NT = ((1,), (1,))


def left_lanes(like):
    return lax.broadcasted_iota(jnp.int32, like.shape, 1) < 64


def swapped_in(a, b):
    left = left_lanes(a)
    return jnp.where(left, a, pltpu.roll(b, 64, 1)), jnp.where(left, pltpu.roll(a, 64, 1), b)


def place(axis, step=0):
    return lax.rem(lax.axis_index(axis) + (2 * SIZE[axis] + step), SIZE[axis])


def mixed(weights, parts):
    total = None
    for weight, part in zip(weights, parts):
        total = weight * part if total is None else total + weight * part
    return total


def along_y_kernel(source, y_vectors, packed, y_high, y_low, rows, vectors, sems):
    copies = [pltpu.make_async_copy(source, rows, sems.at[0])]
    for part in range(4):
        piece = pl.ds(128 * part, 128)
        copies.append(pltpu.make_async_copy(y_vectors.at[piece], vectors.at[piece], sems.at[part + 1]))
    for copy in copies:
        copy.start()
    copies[0].wait()
    high, low = two_parts(rows[...])
    along_y = None
    for part in range(4):
        piece = slice(128 * part, 128 * part + 128)
        copies[part + 1].wait()
        y_high[piece], y_low[piece] = two_parts(vectors[piece])
        term = product((high[:, piece], low[:, piece]), (y_high[piece], y_low[piece]), NN)
        along_y = term if along_y is None else along_y + term
    for g in range(NZ_CHIPS // 2):
        lanes = slice(128 * g, 128 * g + 128)
        even, odd = swapped_in(along_y[:32, lanes], along_y[32:, lanes])
        packed[2 * g] = even
        packed[2 * g + 1] = odd


def divisor_kernel(x_values, z_values, y_values, out, column):
    z = lax.axis_index("z")
    row = lax.axis_index("y") * 8 + lax.axis_index("core") * 4 + lax.axis_index("x")
    of_z = z_values[pl.ds(row, 1), :]
    of_y = y_values[pl.ds(lax.div(z, 2), 1), :]
    column[...] = jnp.broadcast_to(of_y, (128, 128)).T
    of_y = column[pl.ds(pl.multiple_of(lax.rem(z, 2) * 64, 64), 64), :]
    for i in range(4):
        out[64 * i : 64 * i + 64] = (of_z + x_values[i]) + of_y


def half_kernel(first, came, out):
    out[...] = came[first : first + 32]


def forward_kernel(x_vectors, *refs):
    zs, planes, (partial, z_high, z_low, far_high, far_low), (field,) = (
        refs[:7], refs[7:11], refs[11:16], refs[16:]
    )
    z_high[:64] = jnp.zeros((64, 1024), jnp.bfloat16)
    z_low[:64] = jnp.zeros((64, 1024), jnp.bfloat16)
    weights = [[x_vectors[place("y", -s), i] for s in range(4)] for i in range(4)]
    for p, offset in enumerate(OFFSETS):
        rows = slice(64 * p, 64 * p + 64)
        if p:
            z_high[rows], z_low[rows] = two_parts(zs[p - 1][...])
        block = place("z", offset)
        mine = [plane[block] for plane in planes]
        modes = [mixed(weights[i], mine) for i in range(4)]
        for pair in range(2):
            top, bottom = swapped_in(modes[2 * pair], modes[2 * pair + 1])
            lanes = slice(128 * pair, 128 * pair + 128)
            field[64 * p : 64 * p + 32, lanes] = top
            field[64 * p + 32 : 64 * p + 64, lanes] = bottom
    high, low = two_parts(field[...].T)
    far_high[...], far_low[...] = high[:, :128], low[:, :128]
    for tile in range(4):
        lanes = slice(256 * tile, 256 * tile + 256)
        partial[:, lanes] = product((high, low), (z_high[:, lanes], z_low[:, lanes]), NN)


def forward_far_kernel(partial, field_high, field_low, top, bottom, to_partner, kept, far_high, far_low):
    core = lax.axis_index("core")
    far_high[:32], far_low[:32] = two_parts(top[...])
    far_high[32:], far_low[32:] = two_parts(bottom[...])
    field = field_high[:, :64], field_low[:, :64]
    for out, half in ((to_partner, 1 - core), (kept, core)):
        for tile in range(2):
            lanes = pl.ds(pl.multiple_of(half * 512 + tile * 256, 256), 256)
            out[:, 256 * tile : 256 * tile + 256] = partial[:, lanes] + product(
                field, (far_high[:, lanes], far_low[:, lanes]), NN
            )


def by_owner_kernel(kept, received, *outs):
    for s, out in enumerate(outs):
        lanes = pl.ds(pl.multiple_of(place("x", s) * 128, 128), 128)
        out[...] = kept[:, lanes] + received[:, lanes]


def scaled_kernel(a, b, c, d, divisor, out):
    out[...] = ((a[...] + b[...]) + (c[...] + d[...])) / divisor[...]


def backward_kernel(x_vectors, z_high, z_low, far_high, far_low, *refs):
    blocks, outs, (s_high, s_low, first_high, first_low) = refs[:8], refs[8:12], refs[12:]
    for first, far, whole in ((first_high, far_high, z_high), (first_low, far_low, z_low)):
        first[:64] = far[...]
        first[64:] = whole[64:256]
    core = lax.axis_index("core")
    for number, block in enumerate(blocks):
        half = core if number < 4 else 1 - core
        lanes = pl.ds(pl.multiple_of(half * 512 + place("x", -number) * 128, 128), 128)
        s_high[:, lanes], s_low[:, lanes] = two_parts(block[...])
    modes = s_high[...], s_low[...]
    weights = [[x_vectors[place("y", s), i] for i in range(4)] for s in range(4)]
    for p in range(8):
        at = 64 * (p % 4)
        if p == 0:
            part = product((first_high[...], first_low[...]), modes, NT)
        elif p == 4:
            part = product((z_high[256:], z_low[256:]), modes, NT)
        packed = []
        for pair in range(2):
            lanes = slice(128 * pair, 128 * pair + 128)
            packed += swapped_in(part[at : at + 32, lanes], part[at + 32 : at + 64, lanes])
        block = place("z", OFFSETS[p])
        for s, out in enumerate(outs):
            out[block] = mixed(weights[s], packed)


def along_y_back_kernel(packed, y_high, y_low, out, field):
    for g in range(NZ_CHIPS // 2):
        lanes = slice(128 * g, 128 * g + 128)
        field[:32, lanes], field[32:, lanes] = swapped_in(packed[2 * g], packed[2 * g + 1])
    out[...] = product(two_parts(field[...]), (y_high[...], y_low[...]), NT)


def call(kernel, out_shape, operands, smem=0, scratch=(), flops=0, vmem=16 << 20, held=VMEM):
    outs = out_shape if isinstance(out_shape, (tuple, list)) else (out_shape,)
    moved = sum(a.size * a.dtype.itemsize for a in (*operands, *outs))
    return pl.pallas_call(
        kernel,
        out_shape=out_shape,
        in_specs=[SMEM] * smem + [held] * (len(operands) - smem),
        out_specs=VMEM if outs is not out_shape else [VMEM] * len(outs),
        scratch_shapes=list(scratch),
        cost_estimate=pl.CostEstimate(flops=flops, bytes_accessed=moved, transcendentals=0),
        compiler_params=pltpu.CompilerParams(vmem_limit_bytes=vmem),
    )(*operands)


def shards(source, z_vectors, x_vectors, y_vectors, z_values, x_values, y_values):
    packed, y_high, y_low = call(
        along_y_kernel,
        (f32(8, 32, 128), bf16(512, 512), bf16(512, 512)),
        (source, y_vectors),
        flops=2 * 64 * 512 * 512 * 3,
        scratch=[
            pltpu.VMEM((64, 512), jnp.float32),
            pltpu.VMEM((512, 512), jnp.float32),
            pltpu.SemaphoreType.DMA((5,)),
        ],
        held=pl.BlockSpec(memory_space=pltpu.HBM),
        vmem=60 << 20,
    )
    right1 = shifted(z_vectors, "z", 1)
    left1 = shifted(z_vectors, "z", -1)
    plane = lax.all_to_all(packed, "z", 0, 0, tiled=True)
    divisor = call(
        divisor_kernel,
        f32(256, 128),
        (x_values, z_values.reshape(32, 128), y_values.reshape(4, 128)),
        smem=1,
        scratch=[pltpu.VMEM((128, 128), jnp.float32)],
    )
    right2, left2 = shifted(right1, "z", 1), shifted(left1, "z", -1)
    planes = [plane] + [shifted(plane, "y", s) for s in (1, 2, 3)]
    right3, left3 = shifted(right2, "z", 1), shifted(left2, "z", -1)
    top = call(functools.partial(half_kernel, 0), f32(32, 1024), (right3,), vmem=1 << 20)
    bottom = call(functools.partial(half_kernel, 32), f32(32, 1024), (left3,), vmem=1 << 20)
    top, bottom = shifted(top, "z", 1), shifted(bottom, "z", -1)

    partial, z_high, z_low, field_high, field_low = call(
        forward_kernel,
        (f32(256, 1024), bf16(512, 1024), bf16(512, 1024), bf16(256, 128), bf16(256, 128)),
        (x_vectors, z_vectors, right1, right2, right3, left1, left2, left3, *planes),
        smem=1,
        scratch=[pltpu.VMEM((512, 256), jnp.float32)],
        flops=2 * 512 * 256 * 1024 * 3,
    )
    to_partner, kept, far_high, far_low = call(
        forward_far_kernel,
        (f32(256, 512), f32(256, 512), bf16(64, 1024), bf16(64, 1024)),
        (partial, field_high, field_low, top, bottom),
        flops=2 * 64 * 256 * 1024 * 3,
    )
    received = shifted(to_partner, "core", 1)
    mine, *others = call(by_owner_kernel, (f32(256, 128),) * 4, (kept, received))
    sums = [shifted(part, "x", s) for s, part in enumerate(others, 1)]
    scaled = call(scaled_kernel, f32(256, 128), (mine, *sums, divisor))

    modes = [scaled] + [shifted(scaled, "x", s) for s in (1, 2, 3)]
    across = [shifted(block, "core", 1) for block in modes]
    z_parts = z_high, z_low, far_high, far_low
    mine, *others = call(
        backward_kernel,
        (f32(8, 32, 128),) * 4,
        (x_vectors, *z_parts, *modes, *across),
        smem=1,
        scratch=[pltpu.VMEM((256, 1024), jnp.bfloat16)] * 4,
        flops=2 * 512 * 256 * 1024 * 3,
    )
    for s, part in enumerate(others, 1):
        mine = mine + shifted(part, "y", s)
    back = lax.all_to_all(mine, "z", 0, 0, tiled=True)
    return call(
        along_y_back_kernel,
        f32(64, 512),
        (back, y_high, y_low),
        scratch=[pltpu.VMEM((64, 512), jnp.float32)],
        flops=2 * 64 * 512 * 512 * 3,
    )


def solution(mesh):
    devices = mesh.devices.reshape(NZ_CHIPS, NX_CHIPS, CORES, NY_CHIPS)
    torus = Mesh(devices, ("z", "x", "core", "y"))

    return jax.shard_map(
        shards,
        mesh=torus,
        in_specs=(P(GZ, "y"), P(GZ, "y"), P(), P(), P(), P(), P()),
        out_specs=P(GZ, "y"),
        check_vma=False,
    )
```

```python
import functools
import jax
import jax.numpy as jnp
from jax import lax
from jax.experimental import pallas as pl
from jax.experimental.pallas import tpu as pltpu
from jax.sharding import Mesh
from jax.sharding import PartitionSpec as P

NZ_CHIPS, NX_CHIPS, CORES, NY_CHIPS = 8, 4, 2, 4
GZ = ("z", "x", "core")
SIZE = {"z": NZ_CHIPS, "x": NX_CHIPS, "core": CORES, "y": NY_CHIPS}
OFFSETS = (4, 0, -1, -2, -3, 1, 2, 3)


VMEM = pl.BlockSpec(memory_space=pltpu.VMEM)
SMEM = pl.BlockSpec(memory_space=pltpu.SMEM)


def f32(*shape):
    return jax.ShapeDtypeStruct(shape, jnp.float32)


def bf16(*shape):
    return jax.ShapeDtypeStruct(shape, jnp.bfloat16)


def shifted(value, axis, step):
    n = SIZE[axis]
    return lax.ppermute(value, axis, [(i, (i + step) % n) for i in range(n)])


def two_parts(value):
    high = value.astype(jnp.bfloat16)
    return high, (value - high.astype(jnp.float32)).astype(jnp.bfloat16)


def product(left, right, dims):
    one = functools.partial(
        lax.dot_general, dimension_numbers=(dims, ((), ())), preferred_element_type=jnp.float32
    )
    (lh, ll), (rh, rl) = left, right
    return one(lh, rh) + (one(ll, rh) + one(lh, rl))


NN = ((1,), (0,))
NT = ((1,), (1,))


def left_lanes(like):
    return lax.broadcasted_iota(jnp.int32, like.shape, 1) < 64


def swapped_in(a, b):
    left = left_lanes(a)
    return jnp.where(left, a, pltpu.roll(b, 64, 1)), jnp.where(left, pltpu.roll(a, 64, 1), b)


def place(axis, step=0):
    return lax.rem(lax.axis_index(axis) + (2 * SIZE[axis] + step), SIZE[axis])


def mixed(weights, parts):
    total = None
    for weight, part in zip(weights, parts):
        total = weight * part if total is None else total + weight * part
    return total


def along_y_kernel(source, y_vectors, packed, y_high, y_low, rows, vectors, sems):
    copies = [pltpu.make_async_copy(source, rows, sems.at[0])]
    for part in range(4):
        piece = pl.ds(128 * part, 128)
        copies.append(pltpu.make_async_copy(y_vectors.at[piece], vectors.at[piece], sems.at[part + 1]))
    for copy in copies:
        copy.start()
    copies[0].wait()
    high, low = two_parts(rows[...])
    along_y = None
    for part in range(4):
        piece = slice(128 * part, 128 * part + 128)
        copies[part + 1].wait()
        y_high[piece], y_low[piece] = two_parts(vectors[piece])
        term = product((high[:, piece], low[:, piece]), (y_high[piece], y_low[piece]), NN)
        along_y = term if along_y is None else along_y + term
    for g in range(NZ_CHIPS // 2):
        lanes = slice(128 * g, 128 * g + 128)
        even, odd = swapped_in(along_y[:32, lanes], along_y[32:, lanes])
        packed[2 * g] = even
        packed[2 * g + 1] = odd


def divisor_kernel(x_values, z_values, y_values, out, column):
    z = lax.axis_index("z")
    row = lax.axis_index("y") * 8 + lax.axis_index("core") * 4 + lax.axis_index("x")
    of_z = z_values[pl.ds(row, 1), :]
    of_y = y_values[pl.ds(lax.div(z, 2), 1), :]
    column[...] = jnp.broadcast_to(of_y, (128, 128)).T
    of_y = column[pl.ds(pl.multiple_of(lax.rem(z, 2) * 64, 64), 64), :]
    for i in range(4):
        out[64 * i : 64 * i + 64] = (of_z + x_values[i]) + of_y


def turned_kernel(high, low, high_out, low_out):
    high_out[...] = high[...].T
    low_out[...] = low[...].T


def half_kernel(first, came, out):
    out[...] = came[first : first + 32]


def forward_kernel(x_vectors, *refs):
    zs, planes, (partial, z_high, z_low, far_high, far_low), (field,) = (
        refs[:7], refs[7:11], refs[11:16], refs[16:]
    )
    z_high[:64] = jnp.zeros((64, 1024), jnp.bfloat16)
    z_low[:64] = jnp.zeros((64, 1024), jnp.bfloat16)
    weights = [[x_vectors[place("y", -s), i] for s in range(4)] for i in range(4)]
    for p, offset in enumerate(OFFSETS):
        rows = slice(64 * p, 64 * p + 64)
        if p:
            z_high[rows], z_low[rows] = two_parts(zs[p - 1][...])
        block = place("z", offset)
        mine = [plane[block] for plane in planes]
        modes = [mixed(weights[i], mine) for i in range(4)]
        for pair in range(2):
            top, bottom = swapped_in(modes[2 * pair], modes[2 * pair + 1])
            lanes = slice(128 * pair, 128 * pair + 128)
            field[64 * p : 64 * p + 32, lanes] = top
            field[64 * p + 32 : 64 * p + 64, lanes] = bottom
    high, low = two_parts(field[...].T)
    far_high[...], far_low[...] = high[:, :128], low[:, :128]
    for tile in range(4):
        lanes = slice(256 * tile, 256 * tile + 256)
        partial[:, lanes] = product((high, low), (z_high[:, lanes], z_low[:, lanes]), NN)


def far_added(partial, field_high, field_low, far_high, far_low, half, out):
    field = field_high[:, :64], field_low[:, :64]
    for tile in range(2):
        lanes = pl.ds(pl.multiple_of(half * 512 + tile * 256, 256), 256)
        out[:, 256 * tile : 256 * tile + 256] = partial[:, lanes] + product(
            field, (far_high[:, lanes], far_low[:, lanes]), NN
        )


def to_partner_kernel(partial, field_high, field_low, top, bottom, out, far_high, far_low):
    far_high[:32], far_low[:32] = two_parts(top[...])
    far_high[32:], far_low[32:] = two_parts(bottom[...])
    far_added(partial, field_high, field_low, far_high, far_low, 1 - lax.axis_index("core"), out)


def kept_kernel(partial, field_high, field_low, far_high, far_low, out):
    far_added(partial, field_high, field_low, far_high, far_low, lax.axis_index("core"), out)


def by_owner_kernel(kept, received, *outs):
    for s, out in enumerate(outs):
        lanes = pl.ds(pl.multiple_of(place("x", s) * 128, 128), 128)
        out[...] = kept[:, lanes] + received[:, lanes]


def scaled_kernel(a, b, c, d, divisor, out):
    out[...] = ((a[...] + b[...]) + (c[...] + d[...])) / divisor[...]


def half_products(half, z_high, z_low, far_high, far_low, blocks, scratch):
    s_high, s_low, first_high, first_low = scratch
    of_half = pl.ds(pl.multiple_of(half * 512, 512), 512)
    for first, far, whole in ((first_high, far_high, z_high), (first_low, far_low, z_low)):
        first[:64] = far[:, of_half]
        first[64:] = whole[64:256, of_half]
    for s, block in enumerate(blocks):
        lanes = pl.ds(pl.multiple_of(place("x", -s) * 128, 128), 128)
        s_high[:, lanes], s_low[:, lanes] = two_parts(block[...])
    modes = s_high[...], s_low[...]
    yield product((first_high[...], first_low[...]), modes, NT)
    yield product((z_high[256:, of_half], z_low[256:, of_half]), modes, NT)


def backward_own_kernel(z_high, z_low, far_high, far_low, *refs):
    blocks, out, scratch = refs[:4], refs[4], refs[5:]
    half = lax.axis_index("core")
    for number, part in enumerate(half_products(half, z_high, z_low, far_high, far_low, blocks, scratch)):
        out[256 * number : 256 * number + 256] = part


def backward_kernel(x_vectors, own, z_high, z_low, far_high, far_low, *refs):
    blocks, outs, scratch = refs[:4], refs[4:8], refs[8:]
    half = 1 - lax.axis_index("core")
    weights = [[x_vectors[place("y", s), i] for i in range(4)] for s in range(4)]
    for number, part in enumerate(half_products(half, z_high, z_low, far_high, far_low, blocks, scratch)):
        whole = part + own[256 * number : 256 * number + 256]
        for p in range(4):
            packed = []
            for pair in range(2):
                lanes = slice(128 * pair, 128 * pair + 128)
                packed += swapped_in(whole[64 * p : 64 * p + 32, lanes], whole[64 * p + 32 : 64 * p + 64, lanes])
            block = place("z", OFFSETS[4 * number + p])
            for s, out in enumerate(outs):
                out[block] = mixed(weights[s], packed)


def along_y_back_kernel(packed, y_high, y_low, out, field):
    for g in range(NZ_CHIPS // 2):
        lanes = slice(128 * g, 128 * g + 128)
        field[:32, lanes], field[32:, lanes] = swapped_in(packed[2 * g], packed[2 * g + 1])
    out[...] = product(two_parts(field[...]), (y_high[...], y_low[...]), NN)


def call(kernel, out_shape, operands, smem=0, scratch=(), flops=0, vmem=16 << 20, held=VMEM):
    outs = out_shape if isinstance(out_shape, (tuple, list)) else (out_shape,)
    moved = sum(a.size * a.dtype.itemsize for a in (*operands, *outs))
    return pl.pallas_call(
        kernel,
        out_shape=out_shape,
        in_specs=[SMEM] * smem + [held] * (len(operands) - smem),
        out_specs=VMEM if outs is not out_shape else [VMEM] * len(outs),
        scratch_shapes=list(scratch),
        cost_estimate=pl.CostEstimate(flops=flops, bytes_accessed=moved, transcendentals=0),
        compiler_params=pltpu.CompilerParams(vmem_limit_bytes=vmem),
    )(*operands)


def shards(source, z_vectors, x_vectors, y_vectors, z_values, x_values, y_values):
    packed, y_high, y_low = call(
        along_y_kernel,
        (f32(8, 32, 128), bf16(512, 512), bf16(512, 512)),
        (source, y_vectors),
        flops=2 * 64 * 512 * 512 * 3,
        scratch=[
            pltpu.VMEM((64, 512), jnp.float32),
            pltpu.VMEM((512, 512), jnp.float32),
            pltpu.SemaphoreType.DMA((5,)),
        ],
        held=pl.BlockSpec(memory_space=pltpu.HBM),
        vmem=60 << 20,
    )
    right1 = shifted(z_vectors, "z", 1)
    left1 = shifted(z_vectors, "z", -1)
    plane = lax.all_to_all(packed, "z", 0, 0, tiled=True)
    y_high, y_low = call(turned_kernel, (bf16(512, 512),) * 2, (y_high, y_low))
    divisor = call(
        divisor_kernel,
        f32(256, 128),
        (x_values, z_values.reshape(32, 128), y_values.reshape(4, 128)),
        smem=1,
        scratch=[pltpu.VMEM((128, 128), jnp.float32)],
    )
    right2, left2 = shifted(right1, "z", 1), shifted(left1, "z", -1)
    planes = [plane] + [shifted(plane, "y", s) for s in (1, 2, 3)]
    right3, left3 = shifted(right2, "z", 1), shifted(left2, "z", -1)
    top = call(functools.partial(half_kernel, 0), f32(32, 1024), (right3,), vmem=1 << 20)
    bottom = call(functools.partial(half_kernel, 32), f32(32, 1024), (left3,), vmem=1 << 20)
    top, bottom = shifted(top, "z", 1), shifted(bottom, "z", -1)

    partial, z_high, z_low, field_high, field_low = call(
        forward_kernel,
        (f32(256, 1024), bf16(512, 1024), bf16(512, 1024), bf16(256, 128), bf16(256, 128)),
        (x_vectors, z_vectors, right1, right2, right3, left1, left2, left3, *planes),
        smem=1,
        scratch=[pltpu.VMEM((512, 256), jnp.float32)],
        flops=2 * 512 * 256 * 1024 * 3,
    )
    field = field_high, field_low
    to_partner, far_high, far_low = call(
        to_partner_kernel,
        (f32(256, 512), bf16(64, 1024), bf16(64, 1024)),
        (partial, *field, top, bottom),
        flops=64 * 256 * 1024 * 3,
    )
    received = shifted(to_partner, "core", 1)
    kept = call(
        kept_kernel, f32(256, 512), (partial, *field, far_high, far_low), flops=64 * 256 * 1024 * 3
    )
    mine, *others = call(by_owner_kernel, (f32(256, 128),) * 4, (kept, received))
    sums = [shifted(part, "x", s) for s, part in enumerate(others, 1)]
    scaled = call(scaled_kernel, f32(256, 128), (mine, *sums, divisor))

    modes = [scaled] + [shifted(scaled, "x", s) for s in (1, 2, 3)]
    across = [shifted(block, "core", 1) for block in modes]
    z_parts = z_high, z_low, far_high, far_low
    scratch = [pltpu.VMEM((256, 512), jnp.bfloat16)] * 4
    own = call(
        backward_own_kernel,
        f32(512, 256),
        (*z_parts, *modes),
        scratch=scratch,
        flops=512 * 256 * 1024 * 3,
    )
    mine, *others = call(
        backward_kernel,
        (f32(8, 32, 128),) * 4,
        (x_vectors, own, *z_parts, *across),
        smem=1,
        scratch=scratch,
        flops=512 * 256 * 1024 * 3,
    )
    for s, part in enumerate(others, 1):
        mine = mine + shifted(part, "y", s)
    back = lax.all_to_all(mine, "z", 0, 0, tiled=True)
    return call(
        along_y_back_kernel,
        f32(64, 512),
        (back, y_high, y_low),
        scratch=[pltpu.VMEM((64, 512), jnp.float32)],
        flops=2 * 64 * 512 * 512 * 3,
    )


def solution(mesh):
    devices = mesh.devices.reshape(NZ_CHIPS, NX_CHIPS, CORES, NY_CHIPS)
    torus = Mesh(devices, ("z", "x", "core", "y"))

    return jax.shard_map(
        shards,
        mesh=torus,
        in_specs=(P(GZ, "y"), P(GZ, "y"), P(), P(), P(), P(), P()),
        out_specs=P(GZ, "y"),
        check_vma=False,
    )
```

```python
import functools
import jax
import jax.numpy as jnp
from jax import lax
from jax.experimental import pallas as pl
from jax.experimental.pallas import tpu as pltpu
from jax.sharding import Mesh
from jax.sharding import PartitionSpec as P

NZ_CHIPS, NX_CHIPS, CORES, NY_CHIPS = 8, 4, 2, 4
GZ = ("z", "x", "core")
SIZE = {"z": NZ_CHIPS, "x": NX_CHIPS, "core": CORES, "y": NY_CHIPS}
OFFSETS = (4, 0, -1, -2, -3, 1, 2, 3)


VMEM = pl.BlockSpec(memory_space=pltpu.VMEM)
SMEM = pl.BlockSpec(memory_space=pltpu.SMEM)


def f32(*shape):
    return jax.ShapeDtypeStruct(shape, jnp.float32)


def bf16(*shape):
    return jax.ShapeDtypeStruct(shape, jnp.bfloat16)


def shifted(value, axis, step):
    n = SIZE[axis]
    return lax.ppermute(value, axis, [(i, (i + step) % n) for i in range(n)])


def two_parts(value):
    high = value.astype(jnp.bfloat16)
    return high, (value - high.astype(jnp.float32)).astype(jnp.bfloat16)


def product(left, right, dims):
    one = functools.partial(
        lax.dot_general, dimension_numbers=(dims, ((), ())), preferred_element_type=jnp.float32
    )
    (lh, ll), (rh, rl) = left, right
    return one(lh, rh) + (one(ll, rh) + one(lh, rl))


NN = ((1,), (0,))
NT = ((1,), (1,))


def left_lanes(like):
    return lax.broadcasted_iota(jnp.int32, like.shape, 1) < 64


def swapped_in(a, b):
    left = left_lanes(a)
    return jnp.where(left, a, pltpu.roll(b, 64, 1)), jnp.where(left, pltpu.roll(a, 64, 1), b)


def place(axis, step=0):
    return lax.rem(lax.axis_index(axis) + (2 * SIZE[axis] + step), SIZE[axis])


def mixed(weights, parts):
    total = None
    for weight, part in zip(weights, parts):
        total = weight * part if total is None else total + weight * part
    return total


def along_y_kernel(source, y_vectors, packed, y_high, y_low, rows, vectors, sems):
    copies = [pltpu.make_async_copy(source, rows, sems.at[0])]
    for part in range(4):
        piece = pl.ds(128 * part, 128)
        copies.append(pltpu.make_async_copy(y_vectors.at[piece], vectors.at[piece], sems.at[part + 1]))
    for copy in copies:
        copy.start()
    copies[0].wait()
    high, low = two_parts(rows[...])
    along_y = None
    for part in range(4):
        piece = slice(128 * part, 128 * part + 128)
        copies[part + 1].wait()
        y_high[piece], y_low[piece] = two_parts(vectors[piece])
        term = product((high[:, piece], low[:, piece]), (y_high[piece], y_low[piece]), NN)
        along_y = term if along_y is None else along_y + term
    for g in range(NZ_CHIPS // 2):
        lanes = slice(128 * g, 128 * g + 128)
        even, odd = swapped_in(along_y[:32, lanes], along_y[32:, lanes])
        packed[2 * g] = even
        packed[2 * g + 1] = odd


def divisor_kernel(x_values, z_values, y_values, out, column):
    z = lax.axis_index("z")
    row = lax.axis_index("y") * 8 + lax.axis_index("core") * 4 + lax.axis_index("x")
    of_z = z_values[pl.ds(row, 1), :]
    of_y = y_values[pl.ds(lax.div(z, 2), 1), :]
    column[...] = jnp.broadcast_to(of_y, (128, 128)).T
    of_y = column[pl.ds(pl.multiple_of(lax.rem(z, 2) * 64, 64), 64), :]
    for i in range(4):
        out[64 * i : 64 * i + 64] = (of_z + x_values[i]) + of_y


def turned_kernel(high, low, high_out, low_out):
    high_out[...] = high[...].T
    low_out[...] = low[...].T


def half_kernel(first, came, out):
    out[...] = came[first : first + 32]


def forward_kernel(x_vectors, *refs):
    zs, planes, (partial, z_high, z_low, far_high, far_low), (field,) = (
        refs[:7], refs[7:11], refs[11:16], refs[16:]
    )
    z_high[:64] = jnp.zeros((64, 1024), jnp.bfloat16)
    z_low[:64] = jnp.zeros((64, 1024), jnp.bfloat16)
    weights = [[x_vectors[place("y", -s), i] for s in range(4)] for i in range(4)]
    for p, offset in enumerate(OFFSETS):
        rows = slice(64 * p, 64 * p + 64)
        if p:
            z_high[rows], z_low[rows] = two_parts(zs[p - 1][...])
        block = place("z", offset)
        mine = [plane[block] for plane in planes]
        modes = [mixed(weights[i], mine) for i in range(4)]
        for pair in range(2):
            top, bottom = swapped_in(modes[2 * pair], modes[2 * pair + 1])
            lanes = slice(128 * pair, 128 * pair + 128)
            field[64 * p : 64 * p + 32, lanes] = top
            field[64 * p + 32 : 64 * p + 64, lanes] = bottom
    high, low = two_parts(field[...].T)
    far_high[...], far_low[...] = high[:, :128], low[:, :128]
    for tile in range(4):
        lanes = slice(256 * tile, 256 * tile + 256)
        partial[:, lanes] = product((high, low), (z_high[:, lanes], z_low[:, lanes]), NN)


def far_added(partial, field_high, field_low, far_high, far_low, half, out):
    field = field_high[:, :64], field_low[:, :64]
    for tile in range(2):
        lanes = pl.ds(pl.multiple_of(half * 512 + tile * 256, 256), 256)
        out[:, 256 * tile : 256 * tile + 256] = partial[:, lanes] + product(
            field, (far_high[:, lanes], far_low[:, lanes]), NN
        )


def to_partner_kernel(partial, field_high, field_low, top, bottom, out, far_high, far_low):
    far_high[:32], far_low[:32] = two_parts(top[...])
    far_high[32:], far_low[32:] = two_parts(bottom[...])
    far_added(partial, field_high, field_low, far_high, far_low, 1 - lax.axis_index("core"), out)


def kept_kernel(partial, field_high, field_low, far_high, far_low, out):
    far_added(partial, field_high, field_low, far_high, far_low, lax.axis_index("core"), out)


def by_owner_kernel(kept, received, *outs):
    for s, out in enumerate(outs):
        lanes = pl.ds(pl.multiple_of(place("x", s) * 128, 128), 128)
        out[...] = kept[:, lanes] + received[:, lanes]


def scaled_kernel(a, b, c, d, divisor, out):
    out[...] = ((a[...] + b[...]) + (c[...] + d[...])) / divisor[...]


def half_products(half, z_high, z_low, far_high, far_low, blocks, scratch):
    s_high, s_low, first_high, first_low = scratch
    of_half = pl.ds(pl.multiple_of(half * 512, 512), 512)
    for first, far, whole in ((first_high, far_high, z_high), (first_low, far_low, z_low)):
        first[:64] = far[:, of_half]
        first[64:] = whole[64:256, of_half]
    for s, block in enumerate(blocks):
        lanes = pl.ds(pl.multiple_of(place("x", -s) * 128, 128), 128)
        s_high[:, lanes], s_low[:, lanes] = two_parts(block[...])
    modes = s_high[...], s_low[...]
    yield product((first_high[...], first_low[...]), modes, NT)
    yield product((z_high[256:, of_half], z_low[256:, of_half]), modes, NT)


def backward_own_kernel(z_high, z_low, far_high, far_low, *refs):
    blocks, out, scratch = refs[:4], refs[4], refs[5:]
    half = lax.axis_index("core")
    for number, part in enumerate(half_products(half, z_high, z_low, far_high, far_low, blocks, scratch)):
        out[256 * number : 256 * number + 256] = part


def backward_kernel(x_vectors, own, z_high, z_low, far_high, far_low, *refs):
    blocks, outs, scratch = refs[:4], refs[4:8], refs[8:]
    half = 1 - lax.axis_index("core")
    weights = [[x_vectors[place("y", s), i] for i in range(4)] for s in range(4)]
    for number, part in enumerate(half_products(half, z_high, z_low, far_high, far_low, blocks, scratch)):
        whole = part + own[256 * number : 256 * number + 256]
        for p in range(4):
            packed = []
            for pair in range(2):
                lanes = slice(128 * pair, 128 * pair + 128)
                packed += swapped_in(whole[64 * p : 64 * p + 32, lanes], whole[64 * p + 32 : 64 * p + 64, lanes])
            block = place("z", OFFSETS[4 * number + p])
            for s, out in enumerate(outs):
                out[block] = mixed(weights[s], packed)


def summed_kernel(a, b, c, d, out):
    out[...] = (a[...] + b[...]) + (c[...] + d[...])


def along_y_back_kernel(packed, y_high, y_low, out, field):
    for g in range(NZ_CHIPS // 2):
        lanes = slice(128 * g, 128 * g + 128)
        field[:32, lanes], field[32:, lanes] = swapped_in(packed[2 * g], packed[2 * g + 1])
    out[...] = product(two_parts(field[...]), (y_high[...], y_low[...]), NN)


def call(kernel, out_shape, operands, smem=0, scratch=(), flops=0, vmem=16 << 20, held=VMEM):
    outs = out_shape if isinstance(out_shape, (tuple, list)) else (out_shape,)
    moved = sum(a.size * a.dtype.itemsize for a in (*operands, *outs))
    return pl.pallas_call(
        kernel,
        out_shape=out_shape,
        in_specs=[SMEM] * smem + [held] * (len(operands) - smem),
        out_specs=VMEM if outs is not out_shape else [VMEM] * len(outs),
        scratch_shapes=list(scratch),
        cost_estimate=pl.CostEstimate(flops=flops, bytes_accessed=moved, transcendentals=0),
        compiler_params=pltpu.CompilerParams(vmem_limit_bytes=vmem),
    )(*operands)


def shards(source, z_vectors, x_vectors, y_vectors, z_values, x_values, y_values):
    packed, y_high, y_low = call(
        along_y_kernel,
        (f32(8, 32, 128), bf16(512, 512), bf16(512, 512)),
        (source, y_vectors),
        flops=2 * 64 * 512 * 512 * 3,
        scratch=[
            pltpu.VMEM((64, 512), jnp.float32),
            pltpu.VMEM((512, 512), jnp.float32),
            pltpu.SemaphoreType.DMA((5,)),
        ],
        held=pl.BlockSpec(memory_space=pltpu.HBM),
        vmem=60 << 20,
    )
    right1 = shifted(z_vectors, "z", 1)
    left1 = shifted(z_vectors, "z", -1)
    plane = lax.all_to_all(packed, "z", 0, 0, tiled=True)
    y_high, y_low = call(turned_kernel, (bf16(512, 512),) * 2, (y_high, y_low))
    divisor = call(
        divisor_kernel,
        f32(256, 128),
        (x_values, z_values.reshape(32, 128), y_values.reshape(4, 128)),
        smem=1,
        scratch=[pltpu.VMEM((128, 128), jnp.float32)],
    )
    right2, left2 = shifted(right1, "z", 1), shifted(left1, "z", -1)
    planes = [plane] + [shifted(plane, "y", s) for s in (1, 2, 3)]
    right3, left3 = shifted(right2, "z", 1), shifted(left2, "z", -1)
    top = call(functools.partial(half_kernel, 0), f32(32, 1024), (right3,), vmem=1 << 20)
    bottom = call(functools.partial(half_kernel, 32), f32(32, 1024), (left3,), vmem=1 << 20)
    top, bottom = shifted(top, "z", 1), shifted(bottom, "z", -1)

    partial, z_high, z_low, field_high, field_low = call(
        forward_kernel,
        (f32(256, 1024), bf16(512, 1024), bf16(512, 1024), bf16(256, 128), bf16(256, 128)),
        (x_vectors, z_vectors, right1, right2, right3, left1, left2, left3, *planes),
        smem=1,
        scratch=[pltpu.VMEM((512, 256), jnp.float32)],
        flops=2 * 512 * 256 * 1024 * 3,
    )
    field = field_high, field_low
    to_partner, far_high, far_low = call(
        to_partner_kernel,
        (f32(256, 512), bf16(64, 1024), bf16(64, 1024)),
        (partial, *field, top, bottom),
        flops=64 * 256 * 1024 * 3,
    )
    received = shifted(to_partner, "core", 1)
    kept = call(
        kept_kernel, f32(256, 512), (partial, *field, far_high, far_low), flops=64 * 256 * 1024 * 3
    )
    mine, *others = call(by_owner_kernel, (f32(256, 128),) * 4, (kept, received))
    sums = [shifted(part, "x", s) for s, part in enumerate(others, 1)]
    scaled = call(scaled_kernel, f32(256, 128), (mine, *sums, divisor))

    modes = [scaled] + [shifted(scaled, "x", s) for s in (1, 2, 3)]
    across = [shifted(block, "core", 1) for block in modes]
    z_parts = z_high, z_low, far_high, far_low
    scratch = [pltpu.VMEM((256, 512), jnp.bfloat16)] * 4
    own = call(
        backward_own_kernel,
        f32(512, 256),
        (*z_parts, *modes),
        scratch=scratch,
        flops=512 * 256 * 1024 * 3,
    )
    mine, *others = call(
        backward_kernel,
        (f32(8, 32, 128),) * 4,
        (x_vectors, own, *z_parts, *across),
        smem=1,
        scratch=scratch,
        flops=512 * 256 * 1024 * 3,
    )
    others = [shifted(part, "y", s) for s, part in enumerate(others, 1)]
    mine = call(summed_kernel, f32(8, 32, 128), (mine, *others))
    back = lax.all_to_all(mine, "z", 0, 0, tiled=True)
    return call(
        along_y_back_kernel,
        f32(64, 512),
        (back, y_high, y_low),
        scratch=[pltpu.VMEM((64, 512), jnp.float32)],
        flops=2 * 64 * 512 * 512 * 3,
    )


def solution(mesh):
    devices = mesh.devices.reshape(NZ_CHIPS, NX_CHIPS, CORES, NY_CHIPS)
    torus = Mesh(devices, ("z", "x", "core", "y"))

    return jax.shard_map(
        shards,
        mesh=torus,
        in_specs=(P(GZ, "y"), P(GZ, "y"), P(), P(), P(), P(), P()),
        out_specs=P(GZ, "y"),
        check_vma=False,
    )
```

```python
import functools
import jax
import jax.numpy as jnp
from jax import lax
from jax.experimental import pallas as pl
from jax.experimental.pallas import tpu as pltpu
from jax.sharding import Mesh
from jax.sharding import PartitionSpec as P

NZ_CHIPS, NX_CHIPS, CORES, NY_CHIPS = 8, 4, 2, 4
GZ = ("z", "x", "core")
SIZE = {"z": NZ_CHIPS, "x": NX_CHIPS, "core": CORES, "y": NY_CHIPS}
OFFSETS = (4, 0, -1, -2, -3, 1, 2, 3)


VMEM = pl.BlockSpec(memory_space=pltpu.VMEM)
SMEM = pl.BlockSpec(memory_space=pltpu.SMEM)


def f32(*shape):
    return jax.ShapeDtypeStruct(shape, jnp.float32)


def bf16(*shape):
    return jax.ShapeDtypeStruct(shape, jnp.bfloat16)


def shifted(value, axis, step):
    n = SIZE[axis]
    return lax.ppermute(value, axis, [(i, (i + step) % n) for i in range(n)])


def two_parts(value):
    high = value.astype(jnp.bfloat16)
    return high, (value - high.astype(jnp.float32)).astype(jnp.bfloat16)


def product(left, right, dims):
    one = functools.partial(
        lax.dot_general, dimension_numbers=(dims, ((), ())), preferred_element_type=jnp.float32
    )
    (lh, ll), (rh, rl) = left, right
    return one(lh, rh) + (one(ll, rh) + one(lh, rl))


NN = ((1,), (0,))
NT = ((1,), (1,))


def left_lanes(like):
    return lax.broadcasted_iota(jnp.int32, like.shape, 1) < 64


def swapped_in(a, b):
    left = left_lanes(a)
    return jnp.where(left, a, pltpu.roll(b, 64, 1)), jnp.where(left, pltpu.roll(a, 64, 1), b)


def place(axis, step=0):
    return lax.rem(lax.axis_index(axis) + (2 * SIZE[axis] + step), SIZE[axis])


def mixed(weights, parts):
    total = None
    for weight, part in zip(weights, parts):
        total = weight * part if total is None else total + weight * part
    return total


def along_y_kernel(source, y_vectors, packed, y_high, y_low, rows, vectors, sems):
    copies = [pltpu.make_async_copy(source, rows, sems.at[0])]
    for part in range(4):
        piece = pl.ds(128 * part, 128)
        copies.append(pltpu.make_async_copy(y_vectors.at[piece], vectors.at[piece], sems.at[part + 1]))
    for copy in copies:
        copy.start()
    copies[0].wait()
    high, low = two_parts(rows[...])
    along_y = None
    for part in range(4):
        piece = slice(128 * part, 128 * part + 128)
        copies[part + 1].wait()
        y_high[piece], y_low[piece] = two_parts(vectors[piece])
        term = product((high[:, piece], low[:, piece]), (y_high[piece], y_low[piece]), NN)
        along_y = term if along_y is None else along_y + term
    for g in range(NZ_CHIPS // 2):
        lanes = slice(128 * g, 128 * g + 128)
        even, odd = swapped_in(along_y[:32, lanes], along_y[32:, lanes])
        packed[2 * g] = even
        packed[2 * g + 1] = odd


def divisor_kernel(x_values, z_values, y_values, out, column):
    z = lax.axis_index("z")
    row = lax.axis_index("y") * 8 + lax.axis_index("core") * 4 + lax.axis_index("x")
    of_z = z_values[pl.ds(row, 1), :]
    of_y = y_values[pl.ds(lax.div(z, 2), 1), :]
    column[...] = jnp.broadcast_to(of_y, (128, 128)).T
    of_y = column[pl.ds(pl.multiple_of(lax.rem(z, 2) * 64, 64), 64), :]
    for i in range(4):
        out[64 * i : 64 * i + 64] = (of_z + x_values[i]) + of_y


def turned_kernel(high, low, high_out, low_out):
    high_out[...] = high[...].T
    low_out[...] = low[...].T


def part_kernel(first, came, out):
    out[...] = came[first : first + out.shape[0]]


def forward_kernel(x_vectors, *refs):
    zs, planes, (partial, z_high, z_low, far_high, far_low), (field,) = (
        refs[:7], refs[7:11], refs[11:16], refs[16:]
    )
    z_high[:64] = jnp.zeros((64, 1024), jnp.bfloat16)
    z_low[:64] = jnp.zeros((64, 1024), jnp.bfloat16)
    weights = [[x_vectors[place("y", -s), i] for s in range(4)] for i in range(4)]
    for p, offset in enumerate(OFFSETS):
        rows = slice(64 * p, 64 * p + 64)
        if p:
            z_high[rows], z_low[rows] = two_parts(zs[p - 1][...])
        block = place("z", offset)
        mine = [plane[block] for plane in planes]
        modes = [mixed(weights[i], mine) for i in range(4)]
        for pair in range(2):
            top, bottom = swapped_in(modes[2 * pair], modes[2 * pair + 1])
            lanes = slice(128 * pair, 128 * pair + 128)
            field[64 * p : 64 * p + 32, lanes] = top
            field[64 * p + 32 : 64 * p + 64, lanes] = bottom
    high, low = two_parts(field[...].T)
    far_high[...], far_low[...] = high[:, :128], low[:, :128]
    for tile in range(4):
        lanes = slice(256 * tile, 256 * tile + 256)
        partial[:, lanes] = product((high, low), (z_high[:, lanes], z_low[:, lanes]), NN)


def far_added(partial, field_high, field_low, far_high, far_low, half, out):
    field = field_high[:, :64], field_low[:, :64]
    for tile in range(2):
        lanes = pl.ds(pl.multiple_of(half * 512 + tile * 256, 256), 256)
        out[:, 256 * tile : 256 * tile + 256] = partial[:, lanes] + product(
            field, (far_high[:, lanes], far_low[:, lanes]), NN
        )


def to_partner_kernel(partial, field_high, field_low, top, bottom, out, far_high, far_low):
    far_high[:48], far_low[:48] = two_parts(top[...])
    far_high[48:], far_low[48:] = two_parts(bottom[...])
    far_added(partial, field_high, field_low, far_high, far_low, 1 - lax.axis_index("core"), out)


def kept_kernel(partial, field_high, field_low, far_high, far_low, out):
    far_added(partial, field_high, field_low, far_high, far_low, lax.axis_index("core"), out)


def by_owner_kernel(kept, received, *outs):
    for s, out in enumerate(outs):
        lanes = pl.ds(pl.multiple_of(place("x", s) * 128, 128), 128)
        out[...] = kept[:, lanes] + received[:, lanes]


def scaled_kernel(a, b, c, d, divisor, out):
    out[...] = ((a[...] + b[...]) + (c[...] + d[...])) / divisor[...]


def half_products(half, z_high, z_low, far_high, far_low, blocks, scratch):
    s_high, s_low, first_high, first_low = scratch
    of_half = pl.ds(pl.multiple_of(half * 512, 512), 512)
    for first, far, whole in ((first_high, far_high, z_high), (first_low, far_low, z_low)):
        first[:64] = far[:, of_half]
        first[64:] = whole[64:256, of_half]
    for s, block in enumerate(blocks):
        lanes = pl.ds(pl.multiple_of(place("x", -s) * 128, 128), 128)
        s_high[:, lanes], s_low[:, lanes] = two_parts(block[...])
    modes = s_high[...], s_low[...]
    yield product((first_high[...], first_low[...]), modes, NT)
    yield product((z_high[256:, of_half], z_low[256:, of_half]), modes, NT)


def backward_own_kernel(z_high, z_low, far_high, far_low, *refs):
    blocks, out, scratch = refs[:4], refs[4], refs[5:]
    half = lax.axis_index("core")
    for number, part in enumerate(half_products(half, z_high, z_low, far_high, far_low, blocks, scratch)):
        out[256 * number : 256 * number + 256] = part


def backward_kernel(x_vectors, own, z_high, z_low, far_high, far_low, *refs):
    blocks, outs, scratch = refs[:4], refs[4:8], refs[8:]
    half = 1 - lax.axis_index("core")
    weights = [[x_vectors[place("y", s), i] for i in range(4)] for s in range(4)]
    for number, part in enumerate(half_products(half, z_high, z_low, far_high, far_low, blocks, scratch)):
        whole = part + own[256 * number : 256 * number + 256]
        for p in range(4):
            packed = []
            for pair in range(2):
                lanes = slice(128 * pair, 128 * pair + 128)
                packed += swapped_in(whole[64 * p : 64 * p + 32, lanes], whole[64 * p + 32 : 64 * p + 64, lanes])
            block = place("z", OFFSETS[4 * number + p])
            for s, out in enumerate(outs):
                out[block] = mixed(weights[s], packed)


def summed_kernel(a, b, c, d, out):
    out[...] = (a[...] + b[...]) + (c[...] + d[...])


def along_y_back_kernel(packed, y_high, y_low, out, field):
    for g in range(NZ_CHIPS // 2):
        lanes = slice(128 * g, 128 * g + 128)
        field[:32, lanes], field[32:, lanes] = swapped_in(packed[2 * g], packed[2 * g + 1])
    out[...] = product(two_parts(field[...]), (y_high[...], y_low[...]), NN)


def call(kernel, out_shape, operands, smem=0, scratch=(), flops=0, vmem=16 << 20, held=VMEM):
    outs = out_shape if isinstance(out_shape, (tuple, list)) else (out_shape,)
    moved = sum(a.size * a.dtype.itemsize for a in (*operands, *outs))
    return pl.pallas_call(
        kernel,
        out_shape=out_shape,
        in_specs=[SMEM] * smem + [held] * (len(operands) - smem),
        out_specs=VMEM if outs is not out_shape else [VMEM] * len(outs),
        scratch_shapes=list(scratch),
        cost_estimate=pl.CostEstimate(flops=flops, bytes_accessed=moved, transcendentals=0),
        compiler_params=pltpu.CompilerParams(vmem_limit_bytes=vmem),
    )(*operands)


def shards(source, z_vectors, x_vectors, y_vectors, z_values, x_values, y_values):
    packed, y_high, y_low = call(
        along_y_kernel,
        (f32(8, 32, 128), bf16(512, 512), bf16(512, 512)),
        (source, y_vectors),
        flops=2 * 64 * 512 * 512 * 3,
        scratch=[
            pltpu.VMEM((64, 512), jnp.float32),
            pltpu.VMEM((512, 512), jnp.float32),
            pltpu.SemaphoreType.DMA((5,)),
        ],
        held=pl.BlockSpec(memory_space=pltpu.HBM),
        vmem=60 << 20,
    )
    right1 = shifted(z_vectors, "z", 1)
    left1 = shifted(z_vectors, "z", -1)
    plane = lax.all_to_all(packed, "z", 0, 0, tiled=True)
    y_high, y_low = call(turned_kernel, (bf16(512, 512),) * 2, (y_high, y_low))
    divisor = call(
        divisor_kernel,
        f32(256, 128),
        (x_values, z_values.reshape(32, 128), y_values.reshape(4, 128)),
        smem=1,
        scratch=[pltpu.VMEM((128, 128), jnp.float32)],
    )
    right2, left2 = shifted(right1, "z", 1), shifted(left1, "z", -1)
    planes = [plane] + [shifted(plane, "y", s) for s in (1, 2, 3)]
    right3, left3 = shifted(right2, "z", 1), shifted(left2, "z", -1)
    top = call(functools.partial(part_kernel, 0), f32(48, 1024), (right3,), vmem=1 << 20)
    bottom = call(functools.partial(part_kernel, 48), f32(16, 1024), (left3,), vmem=1 << 20)
    top, bottom = shifted(top, "z", 1), shifted(bottom, "z", -1)

    partial, z_high, z_low, field_high, field_low = call(
        forward_kernel,
        (f32(256, 1024), bf16(512, 1024), bf16(512, 1024), bf16(256, 128), bf16(256, 128)),
        (x_vectors, z_vectors, right1, right2, right3, left1, left2, left3, *planes),
        smem=1,
        scratch=[pltpu.VMEM((512, 256), jnp.float32)],
        flops=2 * 512 * 256 * 1024 * 3,
    )
    field = field_high, field_low
    to_partner, far_high, far_low = call(
        to_partner_kernel,
        (f32(256, 512), bf16(64, 1024), bf16(64, 1024)),
        (partial, *field, top, bottom),
        flops=64 * 256 * 1024 * 3,
    )
    received = shifted(to_partner, "core", 1)
    kept = call(
        kept_kernel, f32(256, 512), (partial, *field, far_high, far_low), flops=64 * 256 * 1024 * 3
    )
    mine, *others = call(by_owner_kernel, (f32(256, 128),) * 4, (kept, received))
    sums = [shifted(part, "x", s) for s, part in enumerate(others, 1)]
    scaled = call(scaled_kernel, f32(256, 128), (mine, *sums, divisor))

    modes = [scaled] + [shifted(scaled, "x", s) for s in (1, 2, 3)]
    across = [shifted(block, "core", 1) for block in modes]
    z_parts = z_high, z_low, far_high, far_low
    scratch = [pltpu.VMEM((256, 512), jnp.bfloat16)] * 4
    own = call(
        backward_own_kernel,
        f32(512, 256),
        (*z_parts, *modes),
        scratch=scratch,
        flops=512 * 256 * 1024 * 3,
    )
    mine, *others = call(
        backward_kernel,
        (f32(8, 32, 128),) * 4,
        (x_vectors, own, *z_parts, *across),
        smem=1,
        scratch=scratch,
        flops=512 * 256 * 1024 * 3,
    )
    others = [shifted(part, "y", s) for s, part in enumerate(others, 1)]
    mine = call(summed_kernel, f32(8, 32, 128), (mine, *others))
    back = lax.all_to_all(mine, "z", 0, 0, tiled=True)
    return call(
        along_y_back_kernel,
        f32(64, 512),
        (back, y_high, y_low),
        scratch=[pltpu.VMEM((64, 512), jnp.float32)],
        flops=2 * 64 * 512 * 512 * 3,
    )


def solution(mesh):
    devices = mesh.devices.reshape(NZ_CHIPS, NX_CHIPS, CORES, NY_CHIPS)
    torus = Mesh(devices, ("z", "x", "core", "y"))

    return jax.shard_map(
        shards,
        mesh=torus,
        in_specs=(P(GZ, "y"), P(GZ, "y"), P(), P(), P(), P(), P()),
        out_specs=P(GZ, "y"),
        check_vma=False,
    )
```
